128 devices in a mesh: seq: 128 (over y, x, z, core).
Axes of the slice: x: 4, y: 4, z: 4, core: 2. Of those that a mesh axis runs over, the one named last changes fastest.
Arguments:
- inputs: bfloat16 [16384, 4096], P('seq'), may hold values from -6 to 6
- step_sizes: bfloat16 [16384, 4096], P('seq'), may hold values from 0.25 to 2
- cotangent: bfloat16 [16384, 4096], P('seq'), may hold values from -6 to 6
- input_coeffs: float32 [16, 16384], P(None, 'seq'), may hold values from -0.3 to 0.3
- output_coeffs: float32 [16, 16384], P(None, 'seq'), may hold values from -0.3 to 0.3
- decay_rates: float32 [16, 4096], replicated, as said below
Outputs:
- grad_inputs: bfloat16 [16384, 4096], P('seq')
- grad_steps: bfloat16 [16384, 4096], P('seq')
- grad_in_coeffs: float32 [16, 16384], P(None, 'seq')
- grad_out_coeffs: float32 [16, 16384], P(None, 'seq')
- grad_rates: float32 [16, 4096], P(None, 'seq')
The draws below stay inside these ranges and needn't reach their ends.
Inputs may be any that keep to these rules, and one draw needn't show every extreme that they name: `decay_rates`: every entry lies between 0.1 / 16384 and 0.15.
All inputs are finite; a program needn't handle non-finite values.
Results may differ from the reference program's by a relative error of at most 0.001.
Values sent between devices are 32-bit elements; how exact they have to be, the bound alone decides.
A program may use at most 64 MiB of HBM per device.

```python
import math
from functools import partial
import jax
import jax.numpy as jnp
from jax import lax

CHANNELS = 4096
STATE = 16
TOK_DEV = 128
TOKENS = 16384


def draw_decay_rates(key, part):
    chooser_key, slow_key, fast_key = jax.random.split(jax.random.fold_in(key, 7), 3)
    chooser = jax.random.uniform(chooser_key, (CHANNELS,), jnp.float32)
    fast_rates = jnp.exp(jax.random.uniform(fast_key, (STATE, CHANNELS), jnp.float32, math.log(0.05), math.log(0.15)))
    slow_share = 0.5
    slow_rates = jnp.exp(jax.random.uniform(slow_key, (STATE, CHANNELS), jnp.float32, math.log(0.3), 0.0)) / TOK_DEV
    return jnp.where(chooser[None, :] < slow_share, slow_rates, fast_rates).astype(jnp.float32)


def draw_step_sizes(key, part):
    level_key, jitter_key = jax.random.split(jax.random.fold_in(key, 11), 2)
    run_count = TOKENS // 128
    levels = jax.random.uniform(level_key, (run_count, 1, CHANNELS), jnp.float32, -0.6, 1.2)
    jitter = jax.random.uniform(jitter_key, (run_count, 128, CHANNELS), jnp.float32, -0.5, 0.5)
    values = jnp.clip(0.5 * jnp.exp(levels + jitter), 0.25, 2.0)
    return values.reshape(TOKENS, CHANNELS).astype(jnp.bfloat16)


def block_levels(rng, shape, cuts, least, top_value):
    loudness, own = 1.0, jax.random.fold_in(rng, 6)
    for axis_at, shards_of in cuts:
        heights = jnp.exp(jax.random.uniform(jax.random.fold_in(own, axis_at), (shards_of,), jnp.float32, least / len(cuts), top_value / len(cuts)))
        loudness = loudness * jnp.repeat(heights, shape[axis_at] // shards_of).reshape([-1 if axis == axis_at else 1 for axis in range(len(shape))])
    return loudness


def scatter_about(rng, extent, deviation, reach, cuts=(), dtype=jnp.bfloat16):
    entries = deviation * jax.random.normal(rng, extent, jnp.float32)
    if cuts:
        entries = entries * block_levels(rng, extent, cuts, -0.22, 0.18)
    return jnp.clip(entries, -reach, reach).astype(dtype)


def setup_inputs(seed: int = 0) -> dict:
    key_list = jax.random.split(jax.random.key(seed), 7)
    inputs = scatter_about(key_list[0], (TOKENS, CHANNELS), 1.0, 6.0, ((0, 128),))
    step_sizes = draw_step_sizes(jax.random.fold_in(key_list[6], 71), 0)
    cotangent = scatter_about(key_list[2], (TOKENS, CHANNELS), 1.0, 6.0, ((0, 128),))
    input_coeffs = scatter_about(key_list[3], (STATE, TOKENS), 0.05, 0.3, ((1, 128),), jnp.float32)
    output_coeffs = scatter_about(key_list[4], (STATE, TOKENS), 0.05, 0.3, ((1, 128),), jnp.float32)
    decay_rates = draw_decay_rates(jax.random.fold_in(key_list[6], 71), 0)
    return {"inputs": inputs, "step_sizes": step_sizes, "cotangent": cotangent, "input_coeffs": input_coeffs, "output_coeffs": output_coeffs, "decay_rates": decay_rates}


block_len = 32


def blocked(array):
    return array.reshape(array.shape[0] // block_len, block_len, array.shape[1])


def sweep_forward(initial, inputs, step_sizes, in_rows, decay_rates):
    def per_block(hidden, block_data):
        block_input, block_delta, block_bcoef = block_data
        anchor = hidden
        for position in range(block_len):
            row_delta = block_delta[position].astype(jnp.float32)
            decay_row = jnp.exp(-row_delta[None, :] * decay_rates)
            drive = block_bcoef[position][:, None] * (row_delta * block_input[position].astype(jnp.float32))[None, :]
            hidden = decay_row * hidden + drive
        return hidden, anchor
    return lax.scan(per_block, initial, (blocked(inputs), blocked(step_sizes), blocked(in_rows)))


def block_grads(carried, block_data, decay_rates):
    later, grad_rates = carried
    anchor, block_input, block_delta, block_bcoef, block_ccoef, block_grad = block_data
    hidden_list = [anchor]
    for position in range(block_len):
        row_delta = block_delta[position].astype(jnp.float32)
        decay_row = jnp.exp(-row_delta[None, :] * decay_rates)
        drive = block_bcoef[position][:, None] * (row_delta * block_input[position].astype(jnp.float32))[None, :]
        hidden_list.append(decay_row * hidden_list[-1] + drive)
    input_rows = [None] * block_len
    step_rows = [None] * block_len
    bcoef_rows = [None] * block_len
    ccoef_rows = [None] * block_len
    for position in reversed(range(block_len)):
        row_delta = block_delta[position].astype(jnp.float32)
        row_input = block_input[position].astype(jnp.float32)
        row_grad = block_grad[position].astype(jnp.float32)
        decay_row = jnp.exp(-row_delta[None, :] * decay_rates)
        grad_state = block_ccoef[position][:, None] * row_grad[None, :] + later
        coeff_sum = jnp.sum(grad_state * block_bcoef[position][:, None], 0)
        weighted = grad_state * decay_row * hidden_list[position]
        input_rows[position] = (row_delta * coeff_sum).astype(jnp.bfloat16)
        step_rows[position] = (row_input * coeff_sum - jnp.sum(weighted * decay_rates, 0)).astype(jnp.bfloat16)
        bcoef_rows[position] = jnp.sum(grad_state * (row_delta * row_input)[None, :], 1)
        ccoef_rows[position] = jnp.sum(hidden_list[position + 1] * row_grad[None, :], 1)
        grad_rates = grad_rates - weighted * row_delta[None, :]
        later = decay_row * grad_state
    return (later, grad_rates), (jnp.stack(input_rows), jnp.stack(step_rows), jnp.stack(bcoef_rows), jnp.stack(ccoef_rows))


def reference(inputs, step_sizes, cotangent, input_coeffs, output_coeffs, decay_rates):
    blank = jnp.zeros(decay_rates.shape, jnp.float32)
    in_rows = input_coeffs.T
    out_rows = output_coeffs.T
    _, anchors = sweep_forward(blank, inputs, step_sizes, in_rows, decay_rates)
    block_data = (anchors, blocked(inputs), blocked(step_sizes), blocked(in_rows), blocked(out_rows), blocked(cotangent))
    (_, grad_rates), pieces = lax.scan(partial(block_grads, decay_rates=decay_rates), (blank, blank), block_data, reverse=True)
    channels = inputs.shape[1]
    n_state = decay_rates.shape[0]
    grad_inputs = pieces[0].reshape(-1, channels)
    grad_steps = pieces[1].reshape(-1, channels)
    grad_in_coeffs = pieces[2].reshape(-1, n_state).T
    grad_out_coeffs = pieces[3].reshape(-1, n_state).T
    return (grad_inputs, grad_steps, grad_in_coeffs, grad_out_coeffs, grad_rates)
```

```python
from functools import partial
import math

import jax
import jax.numpy as jnp
from jax import lax
from jax.experimental import pallas as pl
from jax.experimental.pallas import tpu as pltpu
from jax.sharding import PartitionSpec as P

LANES = 128
SUB = 8
TILES = 4
GROUP = 8
PAIR = 16
CHUNKS = 2
LOG2E = math.log2(math.e)
LN2 = math.log(2.0)
F32 = jnp.float32
MESH = pl.DeviceIdType.MESH


def expand(coef_ref, wide, tokens, n_state):
    for t in range(tokens):
        wide[t] = jnp.broadcast_to(coef_ref[:, t : t + 1], (n_state, LANES))


def loop(start, stop, body):
    def step(k, _):
        body(k)
        return 0

    lax.fori_loop(start, stop, step, 0)


def lane_sums(acc, out_ref, tokens, n_state):
    lane = lax.broadcasted_iota(jnp.int32, (n_state, tokens), 1)
    total = jnp.zeros((n_state, tokens), F32)
    for t in range(tokens):
        total = jnp.where(lane == t, jnp.sum(acc[t], axis=1, keepdims=True), total)
    out_ref[...] = total


def whole_kernel(
    n,
    x_ref, d_ref, g_ref, b_ref, c_ref, a_ref,
    gi_ref, gs_ref, gb_ref, gc_ref, gr_ref,
    bx, cx, dl, uu, gg, dec, hs, accb, accc, csp, awp, st, rt, pk,
    out1, in1, out2, in2, out3, in3, send1, recv1, send2, recv2, send3, recv3,
):
    me = lax.axis_index("seq")
    tokens, channels = x_ref.shape
    n_state = a_ref.shape[0]
    all_tiles = channels // LANES
    chunk_tiles = all_tiles // CHUNKS
    chunk_blocks = chunk_tiles // TILES
    owners = n // chunk_tiles
    rows = n_state // owners
    parts = n // all_tiles
    width = LANES // parts
    home = me // (TILES * owners)
    barrier = pltpu.get_barrier_semaphore()

    def tell(k):
        pl.semaphore_signal(barrier, inc=1, device_id=(lax.rem(me + k, n),), device_id_type=MESH)

    def copy(src, dst, send_sem, recv_sem, dest):
        return pltpu.make_async_remote_copy(
            src_ref=src, dst_ref=dst, send_sem=send_sem, recv_sem=recv_sem,
            device_id=(dest,), device_id_type=MESH,
        )

    def settle(ref, sem):
        pltpu.make_async_copy(ref, ref, sem).wait()

    def row(ref, first, t):
        return ref[pl.ds(first, TILES), pl.ds(t, n_state, stride=0), :]

    def lanes_at(tile):
        return pl.ds(pl.multiple_of(tile * LANES, LANES), LANES)

    def rates_of(first):
        for k in range(TILES):
            rt[k] = a_ref[:, lanes_at(first + k)] * (-LOG2E)
        return rt[...]

    loop(1, n, tell)
    expand(b_ref, bx, tokens, n_state)
    expand(c_ref, cx, tokens, n_state)
    accb[...] = jnp.zeros_like(accb)
    accc[...] = jnp.zeros_like(accc)
    state_shape = (TILES, n_state, LANES)
    zero = jnp.zeros(state_shape, F32)

    def first_out(c, dest):
        return out1.at[c, dest, pl.ds(0, 2 * rows + 1)]

    def summarize(c, order):
        b = c * chunk_blocks + lax.rem(home + 1 + order, chunk_blocks)
        first = b * TILES
        for k in range(TILES):
            lanes = lanes_at(first + k)
            delta = d_ref[:, lanes].astype(F32)
            dl[first + k] = delta
            uu[first + k] = delta * x_ref[:, lanes].astype(F32)
            gg[first + k] = g_ref[:, lanes].astype(F32)
        rates = rates_of(first)

        def forth(i, end):
            for s in range(GROUP):
                t = i * GROUP + s
                decay = jnp.exp2(row(dl, first, t) * rates)
                dec[b, t] = decay
                end = decay * end + bx[t][None] * row(uu, first, t)
            return end

        st[0] = lax.fori_loop(0, tokens // GROUP, forth, zero)

        def back(i, later):
            for s in range(GROUP):
                t = tokens - 1 - i * GROUP - s
                later = dec[b, t] * (cx[t][None] * row(gg, first, t) + later)
            return later

        st[1] = lax.fori_loop(0, tokens // GROUP, back, zero)
        for k in range(TILES):
            spent = jnp.sum(dl[first + k], axis=0, keepdims=True)
            for j in range(owners):
                dest = (lax.rem(home + 1 + order, chunk_blocks) * TILES + k) * owners + j
                out1[c, dest, :rows] = st[0, k, j * rows : (j + 1) * rows]
                out1[c, dest, rows : 2 * rows] = st[1, k, j * rows : (j + 1) * rows]
                out1[c, dest, 2 * rows : 2 * rows + 1] = spent

        if c == 0:
            @pl.when(order == 0)
            def _():
                pl.semaphore_wait(barrier, n - 1)

        def send(j):
            dest = lax.rem(home + 1 + order, chunk_blocks) * TILES * owners + j

            @pl.when(dest != me)
            def _():
                copy(
                    first_out(c, dest), in1.at[c, me, pl.ds(0, 2 * rows + 1)],
                    send1.at[c], recv1.at[c], dest,
                ).start()

        loop(0, TILES * owners, send)

    def propagate(c):
        in1[c, me] = out1[c, me]
        settle(in1.at[c, pl.ds(0, n - 1), pl.ds(0, 2 * rows + 1)], recv1.at[c])
        mine = a_ref[:, lanes_at(c * chunk_tiles + me // owners)] * (-LOG2E)
        own = jnp.zeros((rows, LANES), F32)
        for j in range(owners):
            own = jnp.where(lax.rem(me, owners) == j, mine[j * rows : (j + 1) * rows], own)
        own = jnp.concatenate([own, own], axis=0)
        upper = lax.broadcasted_iota(jnp.int32, (2 * rows, LANES), 0) < rows

        def scan(i, state):
            e = n - 1 - i
            out2[c, i, :rows] = state[:rows]
            out2[c, e, rows : 2 * rows] = state[rows:]
            spent = jnp.where(
                upper,
                in1[c, i, pl.ds(2 * rows, 2 * rows, stride=0), :],
                in1[c, e, pl.ds(2 * rows, 2 * rows, stride=0), :],
            )
            term = jnp.where(upper, in1[c, i, : 2 * rows], in1[c, e, : 2 * rows])
            return jnp.exp2(own * spent) * state + term

        lax.fori_loop(0, n, scan, jnp.zeros((2 * rows, LANES), F32), unroll=8)

        def send(k):
            dest = lax.rem(me + n - k, n)
            copy(
                out2.at[c, dest, pl.ds(0, 2 * rows)], in2.at[c, me, pl.ds(0, 2 * rows)],
                send2.at[c], recv2.at[c], dest,
            ).start()

        loop(1, n, send)
        in2[c, me] = out2[c, me]

    lane_group = lax.broadcasted_iota(jnp.int32, (SUB, LANES), 1) // width
    low_lanes = lax.broadcasted_iota(jnp.int32, (SUB // 2, LANES), 1) < LANES // 2

    def differentiate(c, order):
        local = lax.rem(home + order, chunk_blocks)
        b = c * chunk_blocks + local
        first = b * TILES
        for k in range(TILES):
            for j in range(owners):
                origin = (local * TILES + k) * owners + j
                st[0, k, j * rows : (j + 1) * rows] = in2[c, origin, :rows]
                st[1, k, j * rows : (j + 1) * rows] = in2[c, origin, rows : 2 * rows]
        rates = rates_of(first)

        def ahead(i, hidden):
            for s in range(GROUP):
                t = i * GROUP + s
                hs[t] = hidden
                hidden = dec[b, t] * hidden + bx[t][None] * row(uu, first, t)
                accc[t] += jnp.sum(row(gg, first, t) * hidden, axis=0)
            return hidden

        lax.fori_loop(0, tokens // GROUP, ahead, st[0])

        def behind(i, carry):
            later, rate = carry
            base = tokens - PAIR - i * PAIR
            for s in reversed(range(PAIR)):
                t = base + s
                state = cx[t][None] * row(gg, first, t) + later
                later = dec[b, t] * state
                weighted = later * hs[t]
                rate = rate + weighted * row(dl, first, t)
                one, two = state * bx[t][None], weighted * rates
                fold = slice(s * SUB, (s + 1) * SUB)
                csp[:, fold, :] = one[:, :SUB] + one[:, SUB:]
                awp[:, fold, :] = two[:, :SUB] + two[:, SUB:]
                accb[t] += jnp.sum(state * row(uu, first, t), axis=0)
            tok = pl.ds(pl.multiple_of(base, PAIR), PAIR)
            for k in range(TILES):
                coeff = csp[k, pl.ds(0, PAIR, stride=SUB), :]
                weigh = awp[k, pl.ds(0, PAIR, stride=SUB), :]
                for s in range(1, SUB):
                    coeff = coeff + csp[k, pl.ds(s, PAIR, stride=SUB), :]
                    weigh = weigh + awp[k, pl.ds(s, PAIR, stride=SUB), :]
                lanes = lanes_at(first + k)
                x = x_ref[tok, lanes].astype(F32)
                gi_ref[tok, lanes] = (dl[first + k, tok, :] * coeff).astype(gi_ref.dtype)
                gs_ref[tok, lanes] = (x * coeff + LN2 * weigh).astype(gs_ref.dtype)
            return later, rate

        _, rate = lax.fori_loop(0, tokens // PAIR, behind, (st[1], zero))
        for k in range(TILES):
            halves = (-rate[k, :SUB], -rate[k, SUB:])
            turned = [
                [v if s == 0 else pltpu.roll(v, s * width, axis=1) for s in range(parts)]
                for v in halves
            ]
            for j in range(parts):
                packed = turned[0][(0 - j) % parts]
                for g in range(1, parts):
                    packed = jnp.where(lane_group == g, turned[g % 2][(g - j) % parts], packed)
                pk[k * parts + j] = packed
        for k in range(TILES):
            for j in range(parts):
                dest = (first + k) * parts + j
                slot = k * parts + j
                out3[dest] = jnp.where(low_lanes, pk[slot, : SUB // 2], pk[slot, SUB // 2 :])

        def send(j):
            dest = first * parts + j

            @pl.when(dest != me)
            def _():
                copy(out3.at[dest], in3.at[me], send3.at[0], recv3.at[0], dest).start()

        loop(0, TILES * parts, send)

    for c in range(CHUNKS):
        loop(0, chunk_blocks, partial(summarize, c))
    for c in range(CHUNKS):
        propagate(c)
    for c in range(CHUNKS):
        settle(in2.at[c, pl.ds(0, n - 1), pl.ds(0, 2 * rows)], recv2.at[c])
        loop(0, chunk_blocks, partial(differentiate, c))
    in3[me] = out3[me]
    lane_sums(accb, gb_ref, tokens, n_state)
    lane_sums(accc, gc_ref, tokens, n_state)
    settle(in3.at[pl.ds(0, n - 1)], recv3.at[0])
    blank = jnp.zeros((SUB // 2, LANES), F32)
    total = lax.fori_loop(0, n, lambda d, total: total + in3[d], blank, unroll=8)
    gr_ref[0:4, :] = total[:, :width]
    gr_ref[4:8, :] = total[:, 2 * width : 3 * width]
    gr_ref[8:12, :] = total[:, width : 2 * width]
    gr_ref[12:16, :] = total[:, 3 * width :]
    for c in range(CHUNKS):
        settle(out1.at[c, pl.ds(0, n - 1), pl.ds(0, 2 * rows + 1)], send1.at[c])
        settle(out2.at[c, pl.ds(0, n - 1), pl.ds(0, 2 * rows)], send2.at[c])
    settle(out3.at[pl.ds(0, n - 1)], send3.at[0])


def shards(n, inputs, step_sizes, cotangent, input_coeffs, output_coeffs, decay_rates):
    n_state, channels = decay_rates.shape
    tokens = inputs.shape[0]
    all_tiles = channels // LANES
    blocks = all_tiles // TILES
    parts = n // all_tiles
    wide = pltpu.VMEM((tokens, n_state, LANES), F32)
    flat = pltpu.VMEM((all_tiles, tokens, LANES), F32)
    fold = pltpu.VMEM((TILES, PAIR * SUB, LANES), F32)
    vmem = pl.BlockSpec(memory_space=pltpu.VMEM)
    slots = pltpu.VMEM((CHUNKS, n, SUB, LANES), F32)
    small = pltpu.VMEM((n, SUB // 2, LANES), F32)
    each = pltpu.SemaphoreType.DMA((CHUNKS,))
    one = pltpu.SemaphoreType.DMA((1,))
    return pl.pallas_call(
        partial(whole_kernel, n),
        name="whole",
        in_specs=[vmem] * 6,
        out_specs=[vmem] * 5,
        out_shape=[
            jax.ShapeDtypeStruct((tokens, channels), jnp.bfloat16),
            jax.ShapeDtypeStruct((tokens, channels), jnp.bfloat16),
            jax.ShapeDtypeStruct((n_state, tokens), F32),
            jax.ShapeDtypeStruct((n_state, tokens), F32),
            jax.ShapeDtypeStruct((n_state, channels // n), F32),
        ],
        scratch_shapes=[
            wide, wide, flat, flat, flat,
            pltpu.VMEM((blocks, tokens, TILES, n_state, LANES), F32),
            pltpu.VMEM((tokens, TILES, n_state, LANES), F32),
            wide, wide, fold, fold,
            pltpu.VMEM((2, TILES, n_state, LANES), F32),
            pltpu.VMEM((TILES, n_state, LANES), F32),
            pltpu.VMEM((TILES * parts, SUB, LANES), F32),
            slots, slots, slots, slots, small, small,
            each, each, each, each, one, one,
        ],
        compiler_params=pltpu.CompilerParams(
            collective_id=0, has_side_effects=True, vmem_limit_bytes=63 * 1024 * 1024
        ),
    )(inputs, step_sizes, cotangent, input_coeffs, output_coeffs, decay_rates)


def solution(mesh):
    placed = (P("seq", None), P("seq", None), P("seq", None), P(None, "seq"), P(None, "seq"), P())
    return jax.shard_map(
        partial(shards, mesh.shape["seq"]),
        mesh=mesh,
        in_specs=placed,
        out_specs=(P("seq", None), P("seq", None), P(None, "seq"), P(None, "seq"), P(None, "seq")),
        check_vma=False,
    )
```

```python
from functools import partial
import math

import jax
import jax.numpy as jnp
from jax import lax
from jax.experimental import pallas as pl
from jax.experimental.pallas import tpu as pltpu
from jax.sharding import PartitionSpec as P

LANES = 128
SUB = 8
TILES = 4
GROUP = 8
FORTH = 16
BACK = 16
AHEAD = 16
PAIR = 32
CHUNKS = 4
LOG2E = math.log2(math.e)
LN2 = math.log(2.0)
F32 = jnp.float32
MESH = pl.DeviceIdType.MESH


def loop(start, stop, body):
    def step(k, _):
        body(k)
        return 0

    lax.fori_loop(start, stop, step, 0)


def lane_sums(acc, out_ref, tokens, n_state):
    lane = lax.broadcasted_iota(jnp.int32, (n_state, tokens), 1)
    total = jnp.zeros((n_state, tokens), F32)
    for t in range(tokens):
        total = jnp.where(lane == t, jnp.sum(acc[t], axis=1, keepdims=True), total)
    out_ref[...] = total


def whole_kernel(
    n,
    x_hbm, d_hbm, g_hbm, b_hbm, c_hbm, a_hbm,
    giv, gsv, gb_ref, gc_ref, gr_ref,
    xv, dv, gv, bv, cv, av,
    bx, cx, dl, uu, gg, dec, hs, accb, accc, csp, awp, rt, pk,
    out1, in1, out2, in2, out3, in3,
    send1, recv1, send2, recv2, send3, recv3, load, small_load,
):
    me = lax.axis_index("seq")
    tokens, channels = xv.shape
    n_state = av.shape[0]
    all_tiles = channels // LANES
    blocks = all_tiles // TILES
    chunk_tiles = all_tiles // CHUNKS
    chunk_blocks = chunk_tiles // TILES
    parts = n // all_tiles
    width = LANES // parts
    partner = me + 1 - 2 * lax.rem(me, 2)
    barrier = pltpu.get_barrier_semaphore()

    def copy(src, dst, send_sem, recv_sem, dest):
        return pltpu.make_async_remote_copy(
            src_ref=src, dst_ref=dst, send_sem=send_sem, recv_sem=recv_sem,
            device_id=(dest,), device_id_type=MESH,
        )

    def settle(ref, sem):
        pltpu.make_async_copy(ref, ref, sem).wait()

    def row(ref, first, t):
        return ref[pl.ds(first, TILES), pl.ds(t, n_state, stride=0), :]

    def lanes_at(tile, count=1):
        return pl.ds(pl.multiple_of(tile * LANES, LANES), count * LANES)

    def slot(index, count):
        return pl.ds(pl.multiple_of(index * SUB, SUB), count)

    def loads(b):
        lanes = lanes_at(b * TILES, TILES)
        pairs = ((x_hbm, xv), (d_hbm, dv), (g_hbm, gv))
        return [
            pltpu.make_async_copy(src.at[:, lanes], dst.at[:, lanes], load.at[i, b])
            for i, (src, dst) in enumerate(pairs)
        ]

    smalls = [
        pltpu.make_async_copy(src, dst, small_load.at[i])
        for i, (src, dst) in enumerate(((b_hbm, bv), (c_hbm, cv), (a_hbm, av)))
    ]
    for small in smalls:
        small.start()
    for b in range(blocks):
        for each in loads(b):
            each.start()

    def tell(i):
        for k in range(SUB):
            pl.semaphore_signal(
                barrier, inc=1, device_id=(lax.rem(me + 1 + i * SUB + k, n),),
                device_id_type=MESH,
            )

    loop(0, n // SUB, tell)
    for small in smalls[:2]:
        small.wait()
    for t in range(tokens):
        bx[t] = jnp.broadcast_to(bv[:, t : t + 1], (n_state, LANES))
        cx[t] = jnp.broadcast_to(cv[:, t : t + 1], (n_state, LANES))
    smalls[2].wait()
    for k in range(all_tiles):
        rt[k] = av[:, k * LANES : (k + 1) * LANES] * (-LOG2E)

    def clear(i):
        for s in range(GROUP):
            accb[i * GROUP + s] = jnp.zeros((n_state, LANES), F32)
            accc[i * GROUP + s] = jnp.zeros((n_state, LANES), F32)

    loop(0, tokens // GROUP, clear)
    zero = jnp.zeros((TILES, n_state, LANES), F32)

    def other(k):
        far = me + 1 + k
        return jnp.where(far >= n, far - n, far)

    def give1(c, k):
        dest = other(k)
        copy(
            out1.at[c, slot(dest, 3)], in1.at[c, slot(me, 3)], send1.at[c], recv1.at[c], dest
        ).start()

    def give2(c, k):
        dest = other(k)
        copy(
            out2.at[c, slot(dest, 2)], in2.at[c, slot(me, 2)], send2.at[c], recv2.at[c], dest
        ).start()

    def give3(b, k):
        dest = b * TILES * parts + k
        mine = dest == me
        to = jnp.where(mine, partner, dest)
        at = jnp.where(mine, n, me)
        copy(out3.at[dest], in3.at[at], send3.at[0], recv3.at[0], to).start()

    def burst(emit):
        def body(i):
            for s in range(14):
                emit(i * 14 + s)

        loop(0, (n - 2) // 14, body)
        emit(n - 2)

    def summarize(b):
        first = b * TILES
        for each in loads(b):
            each.wait()
        for k in range(TILES):
            lanes = lanes_at(first + k)
            delta = dv[:, lanes].astype(F32)
            dl[first + k] = delta
            uu[first + k] = delta * xv[:, lanes].astype(F32)
            gg[first + k] = gv[:, lanes].astype(F32)

        def forth(i, end):
            rates = rt[pl.ds(first, TILES)]
            for s in range(FORTH):
                t = i * FORTH + s
                decay = jnp.exp2(row(dl, first, t) * rates)
                dec[b, t] = decay
                end = decay * end + bx[t][None] * row(uu, first, t)
            return end

        end = lax.fori_loop(0, tokens // FORTH, forth, zero)
        c = b // chunk_blocks
        base = (b - c * chunk_blocks) * TILES * n_state

        def message(k, r):
            return pl.ds((base + k * n_state) * SUB + r, n_state, stride=SUB)

        for k in range(TILES):
            out1[c, message(k, 0), :] = end[k]
            spent = jnp.sum(dl[first + k], axis=0, keepdims=True)
            out1[c, message(k, 2), :] = jnp.broadcast_to(spent, (n_state, LANES))

        def back(i, later):
            for s in range(BACK):
                t = tokens - 1 - i * BACK - s
                later = dec[b, t] * (cx[t][None] * row(gg, first, t) + later)
            return later

        later = lax.fori_loop(0, tokens // BACK, back, zero)
        for k in range(TILES):
            out1[c, message(k, 1), :] = later[k]

    upper = lax.broadcasted_iota(jnp.int32, (2, LANES), 0) < 1

    def propagate(c):
        settle(in1.at[c, pl.ds(0, 3 * (n - 1))], recv1.at[c])
        in1[c, slot(me, 3), :] = out1[c, slot(me, 3), :]
        own = rt[c * chunk_tiles + me // n_state, pl.ds(lax.rem(me, n_state), 2, stride=0), :]

        def scan(i, state):
            e = n - 1 - i
            out2[c, pl.ds(i * SUB, 1), :] = state[:1]
            out2[c, pl.ds(e * SUB + 1, 1), :] = state[1:]
            spent = jnp.where(
                upper,
                in1[c, pl.ds(i * SUB + 2, 2, stride=0), :],
                in1[c, pl.ds(e * SUB + 2, 2, stride=0), :],
            )
            term = jnp.where(upper, in1[c, slot(i, 2), :], in1[c, slot(e, 2), :])
            return jnp.exp2(own * spent) * state + term

        lax.fori_loop(0, n, scan, jnp.zeros((2, LANES), F32), unroll=8)

    def returned(c):
        settle(in2.at[c, pl.ds(0, 2 * (n - 1))], recv2.at[c])
        in2[c, slot(me, 2), :] = out2[c, slot(me, 2), :]

    lane_group = lax.broadcasted_iota(jnp.int32, (SUB, LANES), 1) // width
    low_lanes = lax.broadcasted_iota(jnp.int32, (SUB // 2, LANES), 1) < LANES // 2

    def differentiate(b):
        first = b * TILES
        c = b // chunk_blocks
        base = (b - c * chunk_blocks) * TILES * n_state

        def incoming(r):
            return jnp.stack([
                in2[c, pl.ds((base + k * n_state) * SUB + r, n_state, stride=SUB), :]
                for k in range(TILES)
            ])

        def ahead(i, hidden):
            for s in range(AHEAD):
                t = i * AHEAD + s
                hs[t] = hidden
                hidden = dec[b, t] * hidden + bx[t][None] * row(uu, first, t)
                accc[t] += jnp.sum(row(gg, first, t) * hidden, axis=0)
            return hidden

        lax.fori_loop(0, tokens // AHEAD, ahead, incoming(0))

        def behind(i, carry):
            later, rate = carry
            rates = rt[pl.ds(first, TILES)]
            start = tokens - PAIR - i * PAIR
            for s in reversed(range(PAIR)):
                t = start + s
                state = cx[t][None] * row(gg, first, t) + later
                later = dec[b, t] * state
                weighted = later * hs[t]
                rate = rate + weighted * row(dl, first, t)
                one, two = state * bx[t][None], weighted * rates
                fold = pl.ds((s // SUB) * SUB * SUB + s % SUB, SUB, stride=SUB)
                for k in range(TILES):
                    csp[k, fold, :] = one[k, :SUB] + one[k, SUB:]
                    awp[k, fold, :] = two[k, :SUB] + two[k, SUB:]
                accb[t] += jnp.sum(state * row(uu, first, t), axis=0)
            tok = pl.ds(pl.multiple_of(start, PAIR), PAIR)

            def folded(ref, k):
                halves = []
                for h in range(PAIR // SUB):
                    pieces = [
                        ref[k, (h * SUB + s) * SUB : (h * SUB + s + 1) * SUB, :]
                        for s in range(SUB)
                    ]
                    while len(pieces) > 1:
                        pieces = [p + q for p, q in zip(pieces[::2], pieces[1::2])]
                    halves.append(pieces[0])
                return jnp.concatenate(halves, axis=0)

            for k in range(TILES):
                coeff, weigh = folded(csp, k), folded(awp, k)
                lanes = lanes_at(first + k)
                x = xv[tok, lanes].astype(F32)
                giv[tok, lanes] = (dl[first + k, tok, :] * coeff).astype(giv.dtype)
                gsv[tok, lanes] = (x * coeff + LN2 * weigh).astype(gsv.dtype)
            return later, rate

        _, rate = lax.fori_loop(0, tokens // PAIR, behind, (incoming(1), zero))
        for k in range(TILES):
            halves = (-rate[k, :SUB], -rate[k, SUB:])
            turned = [
                [v if s == 0 else pltpu.roll(v, s * width, axis=1) for s in range(parts)]
                for v in halves
            ]
            for j in range(parts):
                packed = turned[0][(0 - j) % parts]
                for g in range(1, parts):
                    packed = jnp.where(lane_group == g, turned[g % 2][(g - j) % parts], packed)
                pk[k * parts + j] = packed
        for k in range(TILES):
            for j in range(parts):
                at = k * parts + j
                out3[first * parts + at] = jnp.where(
                    low_lanes, pk[at, : SUB // 2], pk[at, SUB // 2 :]
                )

    for b in range(3):
        summarize(b)
    pl.semaphore_wait(barrier, n)
    burst(partial(give1, 0))
    summarize(3)
    burst(partial(give1, 1))
    for b in range(4, 6):
        summarize(b)
    burst(partial(give1, 2))
    summarize(6)
    propagate(0)
    burst(partial(give2, 0))
    summarize(7)
    burst(partial(give1, 3))
    propagate(1)
    burst(partial(give2, 1))
    propagate(2)
    burst(partial(give2, 2))
    for b in range(blocks):
        if b % chunk_blocks == 0:
            returned(b // chunk_blocks)
        differentiate(b)
        for k in range(TILES * parts):
            give3(b, k)
        if b == 0:
            propagate(3)
            burst(partial(give2, 3))
    in3[me] = out3[me]
    lane_sums(accb, gb_ref, tokens, n_state)
    lane_sums(accc, gc_ref, tokens, n_state)
    settle(in3.at[pl.ds(0, n)], recv3.at[0])
    blank = jnp.zeros((SUB // 2, LANES), F32)
    total = lax.fori_loop(0, n, lambda d, total: total + in3[d], blank, unroll=8)
    gr_ref[0:4, :] = total[:, :width]
    gr_ref[4:8, :] = total[:, 2 * width : 3 * width]
    gr_ref[8:12, :] = total[:, width : 2 * width]
    gr_ref[12:16, :] = total[:, 3 * width :]
    for c in range(CHUNKS):
        settle(out1.at[c, pl.ds(0, 3 * (n - 1))], send1.at[c])
        settle(out2.at[c, pl.ds(0, 2 * (n - 1))], send2.at[c])
    settle(out3.at[pl.ds(0, n)], send3.at[0])


def shards(n, inputs, step_sizes, cotangent, input_coeffs, output_coeffs, decay_rates):
    n_state, channels = decay_rates.shape
    tokens = inputs.shape[0]
    all_tiles = channels // LANES
    blocks = all_tiles // TILES
    parts = n // all_tiles
    wide = pltpu.VMEM((tokens, n_state, LANES), F32)
    flat = pltpu.VMEM((all_tiles, tokens, LANES), F32)
    fold = pltpu.VMEM((TILES, PAIR * SUB, LANES), F32)
    rows = pltpu.VMEM((tokens, channels), jnp.bfloat16)
    coefs = pltpu.VMEM((n_state, tokens), F32)
    vmem = pl.BlockSpec(memory_space=pltpu.VMEM)
    hbm = pl.BlockSpec(memory_space=pl.ANY)
    slots = pltpu.VMEM((CHUNKS, n * SUB, LANES), F32)
    small = pltpu.VMEM((n + 1, SUB // 2, LANES), F32)
    each = pltpu.SemaphoreType.DMA((CHUNKS,))
    one = pltpu.SemaphoreType.DMA((1,))
    outs = [
        jax.ShapeDtypeStruct((tokens, channels), jnp.bfloat16),
        jax.ShapeDtypeStruct((tokens, channels), jnp.bfloat16),
        jax.ShapeDtypeStruct((n_state, tokens), F32),
        jax.ShapeDtypeStruct((n_state, tokens), F32),
        jax.ShapeDtypeStruct((n_state, channels // n), F32),
    ]
    return pl.pallas_call(
        partial(whole_kernel, n),
        name="whole",
        in_specs=[hbm] * 6,
        out_specs=[vmem] * 5,
        out_shape=[pltpu.VMEM(shape.shape, shape.dtype) for shape in outs],
        scratch_shapes=[
            rows, rows, rows, coefs, coefs, pltpu.VMEM((n_state, channels), F32),
            wide, wide, flat, flat, flat,
            pltpu.VMEM((blocks, tokens, TILES, n_state, LANES), F32),
            pltpu.VMEM((tokens, TILES, n_state, LANES), F32),
            wide, wide, fold, fold,
            pltpu.VMEM((all_tiles, n_state, LANES), F32),
            pltpu.VMEM((TILES * parts, SUB, LANES), F32),
            slots, slots, slots, slots, small, small,
            each, each, each, each, one, one,
            pltpu.SemaphoreType.DMA((3, blocks)),
            pltpu.SemaphoreType.DMA((3,)),
        ],
        compiler_params=pltpu.CompilerParams(
            collective_id=0, has_side_effects=True, vmem_limit_bytes=60 * 1024 * 1024
        ),
    )(inputs, step_sizes, cotangent, input_coeffs, output_coeffs, decay_rates)


def solution(mesh):
    placed = (P("seq", None), P("seq", None), P("seq", None), P(None, "seq"), P(None, "seq"), P())
    return jax.shard_map(
        partial(shards, mesh.shape["seq"]),
        mesh=mesh,
        in_specs=placed,
        out_specs=(P("seq", None), P("seq", None), P(None, "seq"), P(None, "seq"), P(None, "seq")),
        check_vma=False,
    )
```

```python
from functools import partial
import math

import jax
import jax.numpy as jnp
from jax import lax
from jax.experimental import pallas as pl
from jax.experimental.pallas import tpu as pltpu
from jax.sharding import PartitionSpec as P

LANES = 128
SUB = 8
TILES = 4
GROUP = 8
FORTH = 32
BACK = 32
AHEAD = 32
PAIR = 32
SWEEP = 32
OCTETS = ((0, 1), (1, 1), (2, 2))
DEFER = 4
LOG2E = math.log2(math.e)
LN2 = math.log(2.0)
F32 = jnp.float32
MESH = pl.DeviceIdType.MESH


def loop(start, stop, body):
    def step(k, _):
        body(k)
        return 0

    lax.fori_loop(start, stop, step, 0)


def lane_sums(acc, out_ref, tokens, n_state):
    lane = lax.broadcasted_iota(jnp.int32, (n_state, tokens), 1)
    total = jnp.zeros((n_state, tokens), F32)
    for t in range(tokens):
        total = jnp.where(lane == t, jnp.sum(acc[t], axis=1, keepdims=True), total)
    out_ref[...] = total


def deliver(*refs):
    sems = refs[-1]
    moves = [
        pltpu.make_async_copy(refs[i], refs[5 + i], sems.at[i]) for i in range(5)
    ]
    for move in moves:
        move.start()
    for move in moves:
        move.wait()


def whole_kernel(
    n,
    x_hbm, d_hbm, g_hbm, b_hbm, c_hbm, a_hbm,
    giv, gsv, gb_ref, gc_ref, gr_ref,
    xv, dv, gv, bv, cv, av,
    bx, cx, dl, uu, gg, dec, hs, accb, accc, csp, awp, rt, rs, pk,
    out1, in1, out2, in2, out3, in3,
    send1, recv1, send2, recv2, send3, recv3, load, small_load,
):
    me = lax.axis_index("seq")
    tokens, channels = xv.shape
    n_state = av.shape[0]
    all_tiles = channels // LANES
    blocks = all_tiles // TILES
    octet = n // n_state
    parts = n // all_tiles
    width = LANES // parts
    partner = me + 1 - 2 * lax.rem(me, 2)
    barrier = pltpu.get_barrier_semaphore()

    def copy(src, dst, send_sem, recv_sem, dest):
        return pltpu.make_async_remote_copy(
            src_ref=src, dst_ref=dst, send_sem=send_sem, recv_sem=recv_sem,
            device_id=(dest,), device_id_type=MESH,
        )

    def other(k):
        far = me + 1 + k
        return jnp.where(far >= n, far - n, far)

    def settle(ref, sem):
        pltpu.make_async_copy(ref, ref, sem).wait()

    def row(ref, first, t):
        return ref[pl.ds(first, TILES), pl.ds(t, n_state, stride=0), :]

    def lanes_at(tile, count=1):
        return pl.ds(pl.multiple_of(tile * LANES, LANES), count * LANES)

    def slot(index, count):
        return pl.ds(pl.multiple_of(index * SUB, SUB), count)

    def loads(b):
        lanes = lanes_at(b * TILES, TILES)
        pairs = ((x_hbm, xv), (d_hbm, dv), (g_hbm, gv))
        return [
            pltpu.make_async_copy(src.at[:, lanes], dst.at[:, lanes], load.at[i, b])
            for i, (src, dst) in enumerate(pairs)
        ]

    smalls = [
        pltpu.make_async_copy(src, dst, small_load.at[i])
        for i, (src, dst) in enumerate(((b_hbm, bv), (c_hbm, cv), (a_hbm, av)))
    ]
    for small in smalls:
        small.start()
    for b in range(blocks):
        for each in loads(b):
            each.start()

    def tell(i):
        for k in range(SUB):
            pl.semaphore_signal(
                barrier, inc=1, device_id=(other(i * SUB + k),),
                device_id_type=MESH,
            )

    loop(0, n // SUB, tell)
    for small in smalls[:2]:
        small.wait()
    for t in range(tokens):
        bx[t] = jnp.broadcast_to(bv[:, t : t + 1], (n_state, LANES))
        cx[t] = jnp.broadcast_to(cv[:, t : t + 1], (n_state, LANES))
    smalls[2].wait()
    for k in range(all_tiles):
        rt[k] = av[:, k * LANES : (k + 1) * LANES] * (-LOG2E)

    def clear(i):
        for s in range(GROUP):
            accb[i * GROUP + s] = jnp.zeros((n_state, LANES), F32)
            accc[i * GROUP + s] = jnp.zeros((n_state, LANES), F32)

    loop(0, tokens // GROUP, clear)
    zero = jnp.zeros((TILES, n_state, LANES), F32)

    def place(b):
        per = octet // TILES
        if isinstance(b, int):
            start = [i for i, (low, count) in enumerate(OCTETS) if low <= b // per][-1]
        else:
            start = len(OCTETS) - 1
        return start, b // per - OCTETS[start][0], lax.rem(b, per) * TILES * n_state

    def give1(c, k):
        dest, rows = other(k), 3 * OCTETS[c][1]
        copy(
            out1.at[c, slot(dest, rows)], in1.at[c, slot(me, rows)],
            send1.at[c], recv1.at[c], dest,
        ).start()

    def give2(c, k):
        dest, rows = other(k), 2 * OCTETS[c][1]
        copy(
            out2.at[c, slot(dest, rows)], in2.at[c, slot(me, rows)],
            send2.at[c], recv2.at[c], dest,
        ).start()

    def give3(k):
        mine = k == me
        to = jnp.where(mine, partner, k)
        at = jnp.where(mine, n, me)
        copy(out3.at[k], in3.at[at], send3.at[0], recv3.at[0], to).start()

    def burst(emit):
        def body(i):
            for s in range(14):
                emit(i * 14 + s)

        loop(0, (n - 2) // 14, body)
        emit(n - 2)

    def summarize(b):
        first = b * TILES
        for each in loads(b):
            each.wait()
        for k in range(TILES):
            lanes = lanes_at(first + k)
            delta = dv[:, lanes].astype(F32)
            dl[first + k] = delta
            uu[first + k] = delta * xv[:, lanes].astype(F32)
            gg[first + k] = gv[:, lanes].astype(F32)

        def forth(i, end):
            rates = rt[pl.ds(first, TILES)]
            for s in range(FORTH):
                t = i * FORTH + s
                decay = jnp.exp2(row(dl, first, t) * rates)
                dec[b, t] = decay
                end = decay * end + bx[t][None] * row(uu, first, t)
            return end

        end = lax.fori_loop(0, tokens // FORTH, forth, zero)
        c, o, base = place(b)
        count = OCTETS[c][1]

        def message(k, r):
            return pl.ds((base + k * n_state) * SUB + r, n_state, stride=SUB)

        for k in range(TILES):
            out1[c, message(k, 2 * o), :] = end[k]
            spent = jnp.sum(dl[first + k], axis=0, keepdims=True)
            out1[c, message(k, 2 * count + o), :] = jnp.broadcast_to(spent, (n_state, LANES))

        def back(i, later):
            for s in range(BACK):
                t = tokens - 1 - i * BACK - s
                later = dec[b, t] * (cx[t][None] * row(gg, first, t) + later)
            return later

        later = lax.fori_loop(0, tokens // BACK, back, zero)
        for k in range(TILES):
            out1[c, message(k, 2 * o + 1), :] = later[k]

    def propagate(c):
        start, count = OCTETS[c]
        run = n // SUB
        settle(in1.at[c, pl.ds(0, 3 * count * (n - 1))], recv1.at[c])
        in1[c, slot(me, 3 * count), :] = out1[c, slot(me, 3 * count), :]
        line = lax.broadcasted_iota(jnp.int32, (SUB, LANES), 0)
        none = jnp.zeros((SUB, LANES), F32)

        def lines(j, r):
            return pl.ds(j * SUB + r, SUB, stride=run * SUB)

        def carried(total, last, shift, edge):
            carry = none
            for _ in range(SUB - 1):
                moved = pltpu.roll(total * carry + last, shift, axis=0)
                carry = jnp.where(line == edge, 0.0, moved)
            return carry

        for o in range(count):
            own = rt[
                (start + o) * octet + me // n_state,
                pl.ds(lax.rem(me, n_state), SUB, stride=0), :
            ]
            decays = [
                jnp.exp2(own * in1[c, lines(j, 2 * count + o), :]) for j in range(run)
            ]
            for r, order, shift, edge in (
                (2 * o, range(run), 1, 0), (2 * o + 1, reversed(range(run)), SUB - 1, SUB - 1)
            ):
                state, product = none, jnp.ones((SUB, LANES), F32)
                kept = []
                for j in order:
                    kept.append((j, state, product))
                    state = decays[j] * state + in1[c, lines(j, r), :]
                    product = decays[j] * product
                carry = carried(product, state, shift, edge)
                for j, local, reach in kept:
                    out2[c, lines(j, r), :] = local + reach * carry

    def returned(c):
        rows = 2 * OCTETS[c][1]
        settle(in2.at[c, pl.ds(0, rows * (n - 1))], recv2.at[c])
        in2[c, slot(me, rows), :] = out2[c, slot(me, rows), :]

    lane_group = lax.broadcasted_iota(jnp.int32, (SUB, LANES), 1) // width
    low_lanes = lax.broadcasted_iota(jnp.int32, (SUB // 2, LANES), 1) < LANES // 2

    def incoming(b, r):
        c, o, base = place(b)
        return jnp.stack([
            in2[c, pl.ds((base + k * n_state) * SUB + 2 * o + r, n_state, stride=SUB), :]
            for k in range(TILES)
        ])

    def restore(b):
        first = b * TILES

        def ahead(i, hidden):
            for s in range(AHEAD):
                t = i * AHEAD + s
                hs[t] = hidden
                hidden = dec[b, t] * hidden + bx[t][None] * row(uu, first, t)
                accc[t] += jnp.sum(row(gg, first, t) * hidden, axis=0)
            return hidden

        lax.fori_loop(0, tokens // AHEAD, ahead, incoming(b, 0))

    def fold_token(first, s, t, state, weighted, rates):
        one, two = state * bx[t][None], weighted * rates
        fold = pl.ds((s // SUB) * SUB * SUB + s % SUB, SUB, stride=SUB)
        for k in range(TILES):
            csp[k, fold, :] = one[k, :SUB] + one[k, SUB:]
            awp[k, fold, :] = two[k, :SUB] + two[k, SUB:]
        accb[t] += jnp.sum(state * row(uu, first, t), axis=0)

    def folded(ref, k):
        halves = []
        for h in range(PAIR // SUB):
            pieces = [
                ref[k, (h * SUB + s) * SUB : (h * SUB + s + 1) * SUB, :] for s in range(SUB)
            ]
            while len(pieces) > 1:
                pieces = [p + q for p, q in zip(pieces[::2], pieces[1::2])]
            halves.append(pieces[0])
        return jnp.concatenate(halves, axis=0)

    def finish(first, start):
        tok = pl.ds(pl.multiple_of(start, PAIR), PAIR)
        for k in range(TILES):
            coeff, weigh = folded(csp, k), folded(awp, k)
            lanes = lanes_at(first + k)
            x = xv[tok, lanes].astype(F32)
            giv[tok, lanes] = (dl[first + k, tok, :] * coeff).astype(giv.dtype)
            gsv[tok, lanes] = (x * coeff + LN2 * weigh).astype(gsv.dtype)

    def differentiate(b):
        first = b * TILES
        restore(b)

        def behind(i, carry):
            later, rate = carry
            rates = rt[pl.ds(first, TILES)]
            start = tokens - PAIR - i * PAIR
            for s in reversed(range(PAIR)):
                t = start + s
                state = cx[t][None] * row(gg, first, t) + later
                later = dec[b, t] * state
                weighted = later * hs[t]
                rate = rate + weighted * row(dl, first, t)
                fold_token(first, s, t, state, weighted, rates)
            finish(first, start)
            return later, rate

        _, rate = lax.fori_loop(0, tokens // PAIR, behind, (incoming(b, 1), zero))
        for k in range(TILES):
            rs[first + k] = -rate[k]

    def sweep(b):
        first = b * TILES
        restore(b)

        def behind(i, carry):
            later, rate = carry
            for s in range(SWEEP):
                t = tokens - 1 - i * SWEEP - s
                state = cx[t][None] * row(gg, first, t) + later
                later = dec[b, t] * state
                weighted = later * hs[t]
                rate = rate + weighted * row(dl, first, t)
                dec[b, t] = state
                dec[b - DEFER, t] = weighted
            return later, rate

        _, rate = lax.fori_loop(0, tokens // SWEEP, behind, (incoming(b, 1), zero))
        for k in range(TILES):
            rs[first + k] = -rate[k]

    def gather(b):
        first = b * TILES

        def body(i):
            rates = rt[pl.ds(first, TILES)]
            start = i * PAIR
            for s in range(PAIR):
                t = start + s
                fold_token(first, s, t, dec[b, t], dec[b - DEFER, t], rates)
            finish(first, start)

        loop(0, tokens // PAIR, body)

    def give_rates(start, stop):
        for tile in range(start * TILES, stop * TILES):
            halves = (rs[tile, :SUB, :], rs[tile, SUB:, :])
            turned = [
                [v if s == 0 else pltpu.roll(v, s * width, axis=1) for s in range(parts)]
                for v in halves
            ]
            for j in range(parts):
                packed = turned[0][(0 - j) % parts]
                for g in range(1, parts):
                    packed = jnp.where(lane_group == g, turned[g % 2][(g - j) % parts], packed)
                pk[(tile - start * TILES) * parts + j] = packed
        for at in range((stop - start) * TILES * parts):
            out3[start * TILES * parts + at] = jnp.where(
                low_lanes, pk[at, : SUB // 2], pk[at, SUB // 2 :]
            )

        def body(i):
            for s in range(16):
                give3(start * TILES * parts + i * 16 + s)

        loop(0, (stop - start) * TILES * parts // 16, body)

    for b in range(3):
        summarize(b)
    pl.semaphore_wait(barrier, n)
    burst(partial(give1, 0))
    summarize(3)
    burst(partial(give1, 1))
    for b in range(4, 6):
        summarize(b)
    summarize(6)
    propagate(0)
    burst(partial(give2, 0))
    summarize(7)
    burst(partial(give1, 2))
    propagate(1)
    burst(partial(give2, 1))
    returned(0)
    differentiate(0)
    differentiate(1)
    propagate(2)
    burst(partial(give2, 2))
    returned(1)
    differentiate(2)
    differentiate(3)
    give_rates(0, DEFER)
    returned(2)
    loop(DEFER, blocks, sweep)
    give_rates(DEFER, blocks)
    loop(DEFER, blocks, gather)
    in3[me] = out3[me]
    lane_sums(accb, gb_ref, tokens, n_state)
    lane_sums(accc, gc_ref, tokens, n_state)
    settle(in3.at[pl.ds(0, n)], recv3.at[0])
    blank = jnp.zeros((SUB // 2, LANES), F32)
    total = lax.fori_loop(0, n, lambda d, total: total + in3[d], blank, unroll=8)
    gr_ref[0:4, :] = total[:, :width]
    gr_ref[4:8, :] = total[:, 2 * width : 3 * width]
    gr_ref[8:12, :] = total[:, width : 2 * width]
    gr_ref[12:16, :] = total[:, 3 * width :]
    for c, (_, count) in enumerate(OCTETS):
        settle(out1.at[c, pl.ds(0, 3 * count * (n - 1))], send1.at[c])
        settle(out2.at[c, pl.ds(0, 2 * count * (n - 1))], send2.at[c])
    settle(out3.at[pl.ds(0, n)], send3.at[0])


def shards(n, inputs, step_sizes, cotangent, input_coeffs, output_coeffs, decay_rates):
    n_state, channels = decay_rates.shape
    tokens = inputs.shape[0]
    all_tiles = channels // LANES
    blocks = all_tiles // TILES
    parts = n // all_tiles
    wide = pltpu.VMEM((tokens, n_state, LANES), F32)
    flat = pltpu.VMEM((all_tiles, tokens, LANES), F32)
    fold = pltpu.VMEM((TILES, PAIR * SUB, LANES), F32)
    rows = pltpu.VMEM((tokens, channels), jnp.bfloat16)
    coefs = pltpu.VMEM((n_state, tokens), F32)
    vmem = pl.BlockSpec(memory_space=pltpu.VMEM)
    hbm = pl.BlockSpec(memory_space=pl.ANY)
    slots = pltpu.VMEM((len(OCTETS), n * SUB, LANES), F32)
    small = pltpu.VMEM((n + 1, SUB // 2, LANES), F32)
    each = pltpu.SemaphoreType.DMA((len(OCTETS),))
    one = pltpu.SemaphoreType.DMA((1,))
    outs = [
        jax.ShapeDtypeStruct((tokens, channels), jnp.bfloat16),
        jax.ShapeDtypeStruct((tokens, channels), jnp.bfloat16),
        jax.ShapeDtypeStruct((n_state, tokens), F32),
        jax.ShapeDtypeStruct((n_state, tokens), F32),
        jax.ShapeDtypeStruct((n_state, channels // n), F32),
    ]
    results = pl.pallas_call(
        partial(whole_kernel, n),
        name="whole",
        in_specs=[hbm] * 6,
        out_specs=[vmem] * 5,
        out_shape=[pltpu.VMEM(shape.shape, shape.dtype) for shape in outs],
        scratch_shapes=[
            rows, rows, rows, coefs, coefs, pltpu.VMEM((n_state, channels), F32),
            wide, wide, flat, flat, flat,
            pltpu.VMEM((blocks, tokens, TILES, n_state, LANES), F32),
            pltpu.VMEM((tokens, TILES, n_state, LANES), F32),
            wide, wide, fold, fold,
            pltpu.VMEM((all_tiles, n_state, LANES), F32),
            pltpu.VMEM((all_tiles, n_state, LANES), F32),
            pltpu.VMEM((DEFER * TILES * parts, SUB, LANES), F32),
            slots, slots, slots, slots, small, small,
            each, each, each, each, one, one,
            pltpu.SemaphoreType.DMA((3, blocks)),
            pltpu.SemaphoreType.DMA((3,)),
        ],
        compiler_params=pltpu.CompilerParams(
            collective_id=0, has_side_effects=True, vmem_limit_bytes=60 * 1024 * 1024
        ),
    )(inputs, step_sizes, cotangent, input_coeffs, output_coeffs, decay_rates)
    return pl.pallas_call(
        deliver,
        name="deliver",
        in_specs=[vmem] * 5,
        out_specs=[hbm] * 5,
        out_shape=outs,
        scratch_shapes=[pltpu.SemaphoreType.DMA((5,))],
        compiler_params=pltpu.CompilerParams(has_side_effects=False, vmem_limit_bytes=1024 * 1024),
    )(*[pltpu.with_memory_space_constraint(r, pltpu.VMEM) for r in results])


def solution(mesh):
    placed = (P("seq", None), P("seq", None), P("seq", None), P(None, "seq"), P(None, "seq"), P())
    return jax.shard_map(
        partial(shards, mesh.shape["seq"]),
        mesh=mesh,
        in_specs=placed,
        out_specs=(P("seq", None), P("seq", None), P(None, "seq"), P(None, "seq"), P(None, "seq")),
        check_vma=False,
    )
```

```python
from functools import partial
import itertools
import math

import jax
import jax.numpy as jnp
from jax import lax
from jax.experimental import pallas as pl
from jax.experimental.pallas import tpu as pltpu
from jax.sharding import PartitionSpec as P

LANES = 128
SUB = 8
TILES = 4
GROUP = 8
FORTH = 32
BACK = 32
AHEAD = 32
PAIR = 32
SWEEP = 32
OCTETS = ((0, 1), (1, 1), (2, 2))
DEFER = 4
LOG2E = math.log2(math.e)
LN2 = math.log(2.0)
F32 = jnp.float32
SIDES = (4, 4, 4, 2)
MESH = pl.DeviceIdType.MESH


def far_first():
    steps = list(itertools.product(*(range(side) for side in SIDES)))
    hops = lambda step: sum(min(s, side - s) for s, side in zip(step[:3], SIDES))
    return sorted(steps[1:], key=hops, reverse=True)


def loop(start, stop, body):
    def step(k, _):
        body(k)
        return 0

    lax.fori_loop(start, stop, step, 0)


def lane_sums(acc, out_ref, tokens, n_state):
    lane = lax.broadcasted_iota(jnp.int32, (n_state, tokens), 1)
    total = jnp.zeros((n_state, tokens), F32)
    for t in range(tokens):
        total = jnp.where(lane == t, jnp.sum(acc[t], axis=1, keepdims=True), total)
    out_ref[...] = total


def deliver(*refs):
    sems = refs[-1]
    moves = [
        pltpu.make_async_copy(refs[i], refs[5 + i], sems.at[i]) for i in range(5)
    ]
    for move in moves:
        move.start()
    for move in moves:
        move.wait()


def whole_kernel(
    n,
    x_hbm, d_hbm, g_hbm, b_hbm, c_hbm, a_hbm,
    giv, gsv, gb_ref, gc_ref, gr_ref,
    xv, dv, gv, bv, cv, av,
    bx, cx, dl, uu, gg, dec, hs, accb, accc, csp, awp, rt, rs, pk,
    out1, in1, out2, in2, out3, in3,
    send1, recv1, send2, recv2, send3, recv3, load, small_load,
):
    me = lax.axis_index("seq")
    tokens, channels = xv.shape
    n_state = av.shape[0]
    all_tiles = channels // LANES
    blocks = all_tiles // TILES
    octet = n // n_state
    parts = n // all_tiles
    width = LANES // parts
    partner = me + 1 - 2 * lax.rem(me, 2)
    barrier = pltpu.get_barrier_semaphore()

    def copy(src, dst, send_sem, recv_sem, dest):
        return pltpu.make_async_remote_copy(
            src_ref=src, dst_ref=dst, send_sem=send_sem, recv_sem=recv_sem,
            device_id=(dest,), device_id_type=MESH,
        )

    moved, stride = [], n
    for side in SIDES:
        stride //= side
        here = lax.rem(me // stride, side)
        moved.append([lax.rem(here + k, side) * stride for k in range(side)])
    planes = [[p + q for q in moved[1]] for p in moved[0]]
    cores = [[p + q for q in moved[3]] for p in moved[2]]

    def everyone(emit):
        for y, x, z, core in far_first():
            emit(planes[y][x] + cores[z][core])

    def settle(ref, sem):
        pltpu.make_async_copy(ref, ref, sem).wait()

    def row(ref, first, t):
        return ref[pl.ds(first, TILES), pl.ds(t, n_state, stride=0), :]

    def lanes_at(tile, count=1):
        return pl.ds(pl.multiple_of(tile * LANES, LANES), count * LANES)

    def slot(index, count):
        return pl.ds(pl.multiple_of(index * SUB, SUB), count)

    def loads(b):
        lanes = lanes_at(b * TILES, TILES)
        pairs = ((x_hbm, xv), (d_hbm, dv), (g_hbm, gv))
        return [
            pltpu.make_async_copy(src.at[:, lanes], dst.at[:, lanes], load.at[i, b])
            for i, (src, dst) in enumerate(pairs)
        ]

    smalls = [
        pltpu.make_async_copy(src, dst, small_load.at[i])
        for i, (src, dst) in enumerate(((b_hbm, bv), (c_hbm, cv), (a_hbm, av)))
    ]
    for small in smalls:
        small.start()
    for b in range(blocks):
        for each in loads(b):
            each.start()

    def tell(dest):
        pl.semaphore_signal(barrier, inc=1, device_id=(dest,), device_id_type=MESH)

    everyone(tell)
    for small in smalls[:2]:
        small.wait()
    for t in range(tokens):
        bx[t] = jnp.broadcast_to(bv[:, t : t + 1], (n_state, LANES))
        cx[t] = jnp.broadcast_to(cv[:, t : t + 1], (n_state, LANES))
    smalls[2].wait()
    for k in range(all_tiles):
        rt[k] = av[:, k * LANES : (k + 1) * LANES] * (-LOG2E)

    zero = jnp.zeros((TILES, n_state, LANES), F32)

    def place(b):
        per = octet // TILES
        if isinstance(b, int):
            start = [i for i, (low, count) in enumerate(OCTETS) if low <= b // per][-1]
        else:
            start = len(OCTETS) - 1
        return start, b // per - OCTETS[start][0], lax.rem(b, per) * TILES * n_state

    def give1(c, dest):
        rows = 3 * OCTETS[c][1]
        copy(
            out1.at[c, slot(dest, rows)], in1.at[c, slot(me, rows)],
            send1.at[c], recv1.at[c], dest,
        ).start()

    def give2(c, dest):
        rows = 2 * OCTETS[c][1]
        copy(
            out2.at[c, slot(dest, rows)], in2.at[c, slot(me, rows)],
            send2.at[c], recv2.at[c], dest,
        ).start()

    def give3(k):
        mine = k == me
        to = jnp.where(mine, partner, k)
        at = jnp.where(mine, n, me)
        copy(out3.at[k], in3.at[at], send3.at[0], recv3.at[0], to).start()

    def summarize(b):
        first = b * TILES
        for each in loads(b):
            each.wait()
        for k in range(TILES):
            lanes = lanes_at(first + k)
            delta = dv[:, lanes].astype(F32)
            dl[first + k] = delta
            uu[first + k] = delta * xv[:, lanes].astype(F32)
            gg[first + k] = gv[:, lanes].astype(F32)

        def forth(i, end):
            rates = rt[pl.ds(first, TILES)]
            for s in range(FORTH):
                t = i * FORTH + s
                decay = jnp.exp2(row(dl, first, t) * rates)
                dec[b, t] = decay
                end = decay * end + bx[t][None] * row(uu, first, t)
            return end

        end = lax.fori_loop(0, tokens // FORTH, forth, zero)
        c, o, base = place(b)
        count = OCTETS[c][1]

        def message(k, r):
            return pl.ds((base + k * n_state) * SUB + r, n_state, stride=SUB)

        for k in range(TILES):
            out1[c, message(k, 2 * o), :] = end[k]
            spent = jnp.sum(dl[first + k], axis=0, keepdims=True)
            out1[c, message(k, 2 * count + o), :] = jnp.broadcast_to(spent, (n_state, LANES))

        def back(i, later):
            for s in range(BACK):
                t = tokens - 1 - i * BACK - s
                later = dec[b, t] * (cx[t][None] * row(gg, first, t) + later)
            return later

        later = lax.fori_loop(0, tokens // BACK, back, zero)
        for k in range(TILES):
            out1[c, message(k, 2 * o + 1), :] = later[k]

    def propagate(c):
        start, count = OCTETS[c]
        run = n // SUB
        settle(in1.at[c, pl.ds(0, 3 * count * (n - 1))], recv1.at[c])
        in1[c, slot(me, 3 * count), :] = out1[c, slot(me, 3 * count), :]
        line = lax.broadcasted_iota(jnp.int32, (SUB, LANES), 0)
        none = jnp.zeros((SUB, LANES), F32)

        def lines(j, r):
            return pl.ds(j * SUB + r, SUB, stride=run * SUB)

        def carried(total, last, shift, edge):
            carry = none
            for _ in range(SUB - 1):
                moved = pltpu.roll(total * carry + last, shift, axis=0)
                carry = jnp.where(line == edge, 0.0, moved)
            return carry

        for o in range(count):
            own = rt[
                (start + o) * octet + me // n_state,
                pl.ds(lax.rem(me, n_state), SUB, stride=0), :
            ]
            decays = [
                jnp.exp2(own * in1[c, lines(j, 2 * count + o), :]) for j in range(run)
            ]
            for r, order, shift, edge in (
                (2 * o, range(run), 1, 0), (2 * o + 1, reversed(range(run)), SUB - 1, SUB - 1)
            ):
                state, product = none, jnp.ones((SUB, LANES), F32)
                kept = []
                for j in order:
                    kept.append((j, state, product))
                    state = decays[j] * state + in1[c, lines(j, r), :]
                    product = decays[j] * product
                carry = carried(product, state, shift, edge)
                for j, local, reach in kept:
                    out2[c, lines(j, r), :] = local + reach * carry

    def returned(c):
        rows = 2 * OCTETS[c][1]
        settle(in2.at[c, pl.ds(0, rows * (n - 1))], recv2.at[c])
        in2[c, slot(me, rows), :] = out2[c, slot(me, rows), :]

    lane_group = lax.broadcasted_iota(jnp.int32, (SUB, LANES), 1) // width
    low_lanes = lax.broadcasted_iota(jnp.int32, (SUB // 2, LANES), 1) < LANES // 2

    def incoming(b, r):
        c, o, base = place(b)
        return jnp.stack([
            in2[c, pl.ds((base + k * n_state) * SUB + 2 * o + r, n_state, stride=SUB), :]
            for k in range(TILES)
        ])

    def gain(acc, t, part, fresh):
        acc[t] = part if fresh else acc[t] + part

    def restore(b):
        first = b * TILES
        fresh = isinstance(b, int) and b == 0

        def ahead(i, hidden):
            for s in range(AHEAD):
                t = i * AHEAD + s
                hs[t] = hidden
                hidden = dec[b, t] * hidden + bx[t][None] * row(uu, first, t)
                gain(accc, t, jnp.sum(row(gg, first, t) * hidden, axis=0), fresh)
            return hidden

        lax.fori_loop(0, tokens // AHEAD, ahead, incoming(b, 0))

    def fold_token(first, s, t, state, weighted, rates, fresh=False):
        one, two = state * bx[t][None], weighted * rates
        fold = pl.ds((s // SUB) * SUB * SUB + s % SUB, SUB, stride=SUB)
        for k in range(TILES):
            csp[k, fold, :] = one[k, :SUB] + one[k, SUB:]
            awp[k, fold, :] = two[k, :SUB] + two[k, SUB:]
        gain(accb, t, jnp.sum(state * row(uu, first, t), axis=0), fresh)

    def folded(ref, k):
        halves = []
        for h in range(PAIR // SUB):
            pieces = [
                ref[k, (h * SUB + s) * SUB : (h * SUB + s + 1) * SUB, :] for s in range(SUB)
            ]
            while len(pieces) > 1:
                pieces = [p + q for p, q in zip(pieces[::2], pieces[1::2])]
            halves.append(pieces[0])
        return jnp.concatenate(halves, axis=0)

    def finish(first, start):
        tok = pl.ds(pl.multiple_of(start, PAIR), PAIR)
        for k in range(TILES):
            coeff, weigh = folded(csp, k), folded(awp, k)
            lanes = lanes_at(first + k)
            x = xv[tok, lanes].astype(F32)
            giv[tok, lanes] = (dl[first + k, tok, :] * coeff).astype(giv.dtype)
            gsv[tok, lanes] = (x * coeff + LN2 * weigh).astype(gsv.dtype)

    def differentiate(b):
        first = b * TILES
        restore(b)

        def behind(i, carry):
            later, rate = carry
            rates = rt[pl.ds(first, TILES)]
            start = tokens - PAIR - i * PAIR
            for s in reversed(range(PAIR)):
                t = start + s
                state = cx[t][None] * row(gg, first, t) + later
                later = dec[b, t] * state
                weighted = later * hs[t]
                rate = rate + weighted * row(dl, first, t)
                fold_token(first, s, t, state, weighted, rates, first == 0)
            finish(first, start)
            return later, rate

        _, rate = lax.fori_loop(0, tokens // PAIR, behind, (incoming(b, 1), zero))
        for k in range(TILES):
            rs[first + k] = -rate[k]

    def sweep(b):
        first = b * TILES
        restore(b)

        def behind(i, carry):
            later, rate = carry
            for s in range(SWEEP):
                t = tokens - 1 - i * SWEEP - s
                state = cx[t][None] * row(gg, first, t) + later
                later = dec[b, t] * state
                weighted = later * hs[t]
                rate = rate + weighted * row(dl, first, t)
                dec[b, t] = state
                dec[b - DEFER, t] = weighted
            return later, rate

        _, rate = lax.fori_loop(0, tokens // SWEEP, behind, (incoming(b, 1), zero))
        for k in range(TILES):
            rs[first + k] = -rate[k]

    def gather(b):
        first = b * TILES

        def body(i):
            rates = rt[pl.ds(first, TILES)]
            start = i * PAIR
            for s in range(PAIR):
                t = start + s
                fold_token(first, s, t, dec[b, t], dec[b - DEFER, t], rates)
            finish(first, start)

        loop(0, tokens // PAIR, body)

    def give_rates(start, stop):
        for tile in range(start * TILES, stop * TILES):
            halves = (rs[tile, :SUB, :], rs[tile, SUB:, :])
            turned = [
                [v if s == 0 else pltpu.roll(v, s * width, axis=1) for s in range(parts)]
                for v in halves
            ]
            for j in range(parts):
                packed = turned[0][(0 - j) % parts]
                for g in range(1, parts):
                    packed = jnp.where(lane_group == g, turned[g % 2][(g - j) % parts], packed)
                pk[(tile - start * TILES) * parts + j] = packed
        for at in range((stop - start) * TILES * parts):
            out3[start * TILES * parts + at] = jnp.where(
                low_lanes, pk[at, : SUB // 2], pk[at, SUB // 2 :]
            )

        for at in range((stop - start) * TILES * parts):
            give3(start * TILES * parts + at)

    for b in range(4):
        summarize(b)
    pl.semaphore_wait(barrier, n - 1)
    everyone(partial(give1, 0))
    everyone(partial(give1, 1))
    for b in range(4, 7):
        summarize(b)
    propagate(0)
    everyone(partial(give2, 0))
    summarize(7)
    everyone(partial(give1, 2))
    propagate(1)
    everyone(partial(give2, 1))
    returned(0)
    differentiate(0)
    differentiate(1)
    propagate(2)
    everyone(partial(give2, 2))
    returned(1)
    differentiate(2)
    differentiate(3)
    give_rates(0, DEFER)
    returned(2)
    loop(DEFER, blocks, sweep)
    give_rates(DEFER, blocks)
    loop(DEFER, blocks, gather)
    in3[me] = out3[me]
    lane_sums(accb, gb_ref, tokens, n_state)
    lane_sums(accc, gc_ref, tokens, n_state)
    settle(in3.at[pl.ds(0, n)], recv3.at[0])
    blank = jnp.zeros((SUB // 2, LANES), F32)
    total = lax.fori_loop(0, n, lambda d, total: total + in3[d], blank, unroll=8)
    gr_ref[0:4, :] = total[:, :width]
    gr_ref[4:8, :] = total[:, 2 * width : 3 * width]
    gr_ref[8:12, :] = total[:, width : 2 * width]
    gr_ref[12:16, :] = total[:, 3 * width :]
    for c, (_, count) in enumerate(OCTETS):
        settle(out1.at[c, pl.ds(0, 3 * count * (n - 1))], send1.at[c])
        settle(out2.at[c, pl.ds(0, 2 * count * (n - 1))], send2.at[c])
    settle(out3.at[pl.ds(0, n)], send3.at[0])


def shards(n, inputs, step_sizes, cotangent, input_coeffs, output_coeffs, decay_rates):
    n_state, channels = decay_rates.shape
    tokens = inputs.shape[0]
    all_tiles = channels // LANES
    blocks = all_tiles // TILES
    parts = n // all_tiles
    wide = pltpu.VMEM((tokens, n_state, LANES), F32)
    flat = pltpu.VMEM((all_tiles, tokens, LANES), F32)
    fold = pltpu.VMEM((TILES, PAIR * SUB, LANES), F32)
    rows = pltpu.VMEM((tokens, channels), jnp.bfloat16)
    coefs = pltpu.VMEM((n_state, tokens), F32)
    vmem = pl.BlockSpec(memory_space=pltpu.VMEM)
    hbm = pl.BlockSpec(memory_space=pl.ANY)
    slots = pltpu.VMEM((len(OCTETS), n * SUB, LANES), F32)
    small = pltpu.VMEM((n + 1, SUB // 2, LANES), F32)
    each = pltpu.SemaphoreType.DMA((len(OCTETS),))
    one = pltpu.SemaphoreType.DMA((1,))
    outs = [
        jax.ShapeDtypeStruct((tokens, channels), jnp.bfloat16),
        jax.ShapeDtypeStruct((tokens, channels), jnp.bfloat16),
        jax.ShapeDtypeStruct((n_state, tokens), F32),
        jax.ShapeDtypeStruct((n_state, tokens), F32),
        jax.ShapeDtypeStruct((n_state, channels // n), F32),
    ]
    results = pl.pallas_call(
        partial(whole_kernel, n),
        name="whole",
        in_specs=[hbm] * 6,
        out_specs=[vmem] * 5,
        out_shape=[pltpu.VMEM(shape.shape, shape.dtype) for shape in outs],
        scratch_shapes=[
            rows, rows, rows, coefs, coefs, pltpu.VMEM((n_state, channels), F32),
            wide, wide, flat, flat, flat,
            pltpu.VMEM((blocks, tokens, TILES, n_state, LANES), F32),
            pltpu.VMEM((tokens, TILES, n_state, LANES), F32),
            wide, wide, fold, fold,
            pltpu.VMEM((all_tiles, n_state, LANES), F32),
            pltpu.VMEM((all_tiles, n_state, LANES), F32),
            pltpu.VMEM((DEFER * TILES * parts, SUB, LANES), F32),
            slots, slots, slots, slots, small, small,
            each, each, each, each, one, one,
            pltpu.SemaphoreType.DMA((3, blocks)),
            pltpu.SemaphoreType.DMA((3,)),
        ],
        compiler_params=pltpu.CompilerParams(
            collective_id=0, has_side_effects=True, vmem_limit_bytes=60 * 1024 * 1024
        ),
    )(inputs, step_sizes, cotangent, input_coeffs, output_coeffs, decay_rates)
    return pl.pallas_call(
        deliver,
        name="deliver",
        in_specs=[vmem] * 5,
        out_specs=[hbm] * 5,
        out_shape=outs,
        scratch_shapes=[pltpu.SemaphoreType.DMA((5,))],
        compiler_params=pltpu.CompilerParams(has_side_effects=False, vmem_limit_bytes=1024 * 1024),
    )(*[pltpu.with_memory_space_constraint(r, pltpu.VMEM) for r in results])


def solution(mesh):
    placed = (P("seq", None), P("seq", None), P("seq", None), P(None, "seq"), P(None, "seq"), P())
    return jax.shard_map(
        partial(shards, mesh.shape["seq"]),
        mesh=mesh,
        in_specs=placed,
        out_specs=(P("seq", None), P("seq", None), P(None, "seq"), P(None, "seq"), P(None, "seq")),
        check_vma=False,
    )
```

```python
from functools import partial
import itertools
import math

import jax
import jax.numpy as jnp
from jax import lax
from jax.experimental import pallas as pl
from jax.experimental.pallas import tpu as pltpu
from jax.sharding import PartitionSpec as P

LANES = 128
SUB = 8
TILES = 4
GROUP = 8
FORTH = 32
BACK = 32
AHEAD = 32
PAIR = 32
SWEEP = 32
OCTETS = ((0, 1), (1, 1), (2, 2))
DEFER = 4
LOG2E = math.log2(math.e)
LN2 = math.log(2.0)
F32 = jnp.float32
SIDES = (4, 4, 4, 2)
PIECES = 4
MESH = pl.DeviceIdType.MESH


def far_first():
    steps = list(itertools.product(*(range(side) for side in SIDES)))
    hops = lambda step: sum(min(s, side - s) for s, side in zip(step[:3], SIDES))
    return sorted(steps[1:], key=hops, reverse=True)


def loop(start, stop, body):
    def step(k, _):
        body(k)
        return 0

    lax.fori_loop(start, stop, step, 0)


def lane_sums(acc, out_ref, tokens, n_state):
    lane = lax.broadcasted_iota(jnp.int32, (n_state, tokens), 1)
    total = jnp.zeros((n_state, tokens), F32)
    for t in range(tokens):
        total = jnp.where(lane == t, jnp.sum(acc[t], axis=1, keepdims=True), total)
    out_ref[...] = total


def deliver(*refs):
    sems = refs[-1]
    moves = []
    for i in range(5):
        pieces = PIECES if i < 2 else 1
        rows = refs[i].shape[0] // pieces
        for p in range(pieces):
            part = pl.ds(p * rows, rows)
            moves.append(
                pltpu.make_async_copy(refs[i].at[part], refs[5 + i].at[part], sems.at[i, p])
            )
    for move in moves:
        move.start()
    for move in moves:
        move.wait()


def whole_kernel(
    n,
    x_hbm, d_hbm, g_hbm, b_hbm, c_hbm, a_hbm,
    giv, gsv, gb_ref, gc_ref, gr_ref,
    xv, dv, gv, bv, cv, av,
    bx, cx, dl, uu, gg, dec, hs, accb, accc, csp, awp, rt, rs, pk,
    out1, in1, out2, in2, out3, in3,
    send1, recv1, send2, recv2, send3, recv3, load, small_load,
):
    me = lax.axis_index("seq")
    tokens, channels = xv.shape
    n_state = av.shape[0]
    all_tiles = channels // LANES
    blocks = all_tiles // TILES
    octet = n // n_state
    parts = n // all_tiles
    width = LANES // parts
    partner = me + 1 - 2 * lax.rem(me, 2)
    barrier = pltpu.get_barrier_semaphore()

    def copy(src, dst, send_sem, recv_sem, dest):
        return pltpu.make_async_remote_copy(
            src_ref=src, dst_ref=dst, send_sem=send_sem, recv_sem=recv_sem,
            device_id=(dest,), device_id_type=MESH,
        )

    moved, stride = [], n
    for side in SIDES:
        stride //= side
        here = lax.rem(me // stride, side)
        moved.append([lax.rem(here + k, side) * stride for k in range(side)])
    planes = [[p + q for q in moved[1]] for p in moved[0]]
    cores = [[p + q for q in moved[3]] for p in moved[2]]

    def everyone(emit):
        for y, x, z, core in far_first():
            emit(planes[y][x] + cores[z][core])

    def settle(ref, sem):
        pltpu.make_async_copy(ref, ref, sem).wait()

    def row(ref, first, t):
        return ref[pl.ds(first, TILES), pl.ds(t, n_state, stride=0), :]

    def lanes_at(tile, count=1):
        return pl.ds(pl.multiple_of(tile * LANES, LANES), count * LANES)

    def slot(index, count):
        return pl.ds(pl.multiple_of(index * SUB, SUB), count)

    def loads(b):
        lanes = lanes_at(b * TILES, TILES)
        pairs = ((x_hbm, xv), (d_hbm, dv), (g_hbm, gv))
        return [
            pltpu.make_async_copy(src.at[:, lanes], dst.at[:, lanes], load.at[i, b])
            for i, (src, dst) in enumerate(pairs)
        ]

    smalls = [
        pltpu.make_async_copy(src, dst, small_load.at[i])
        for i, (src, dst) in enumerate(((b_hbm, bv), (c_hbm, cv), (a_hbm, av)))
    ]
    for small in smalls:
        small.start()
    for b in range(blocks):
        for each in loads(b):
            each.start()

    def tell(dest):
        pl.semaphore_signal(barrier, inc=1, device_id=(dest,), device_id_type=MESH)

    everyone(tell)
    for small in smalls[:2]:
        small.wait()
    for t in range(tokens):
        bx[t] = jnp.broadcast_to(bv[:, t : t + 1], (n_state, LANES))
        cx[t] = jnp.broadcast_to(cv[:, t : t + 1], (n_state, LANES))
    smalls[2].wait()
    for k in range(all_tiles):
        rt[k] = av[:, k * LANES : (k + 1) * LANES] * (-LOG2E)

    zero = jnp.zeros((TILES, n_state, LANES), F32)

    def place(b):
        per = octet // TILES
        if isinstance(b, int):
            start = [i for i, (low, count) in enumerate(OCTETS) if low <= b // per][-1]
        else:
            start = len(OCTETS) - 1
        return start, b // per - OCTETS[start][0], lax.rem(b, per) * TILES * n_state

    def give1(c, dest):
        rows = 3 * OCTETS[c][1]
        copy(
            out1.at[c, slot(dest, rows)], in1.at[c, slot(me, rows)],
            send1.at[c], recv1.at[c], dest,
        ).start()

    def give2(c, dest):
        rows = 2 * OCTETS[c][1]
        copy(
            out2.at[c, slot(dest, rows)], in2.at[c, slot(me, rows)],
            send2.at[c], recv2.at[c], dest,
        ).start()

    def give3(k):
        mine = k == me
        to = jnp.where(mine, partner, k)
        at = jnp.where(mine, n, me)
        copy(out3.at[k], in3.at[at], send3.at[0], recv3.at[0], to).start()

    def summarize(b):
        first = b * TILES
        for each in loads(b):
            each.wait()
        for k in range(TILES):
            lanes = lanes_at(first + k)
            delta = dv[:, lanes].astype(F32)
            dl[first + k] = delta
            uu[first + k] = delta * xv[:, lanes].astype(F32)
            gg[first + k] = gv[:, lanes].astype(F32)

        def forth(i, end):
            rates = rt[pl.ds(first, TILES)]
            for s in range(FORTH):
                t = i * FORTH + s
                decay = jnp.exp2(row(dl, first, t) * rates)
                dec[b, t] = decay
                end = decay * end + bx[t][None] * row(uu, first, t)
            return end

        end = lax.fori_loop(0, tokens // FORTH, forth, zero)
        c, o, base = place(b)
        count = OCTETS[c][1]

        def message(k, r):
            return pl.ds((base + k * n_state) * SUB + r, n_state, stride=SUB)

        for k in range(TILES):
            out1[c, message(k, 2 * o), :] = end[k]
            spent = jnp.sum(dl[first + k], axis=0, keepdims=True)
            out1[c, message(k, 2 * count + o), :] = jnp.broadcast_to(spent, (n_state, LANES))

        def back(i, later):
            for s in range(BACK):
                t = tokens - 1 - i * BACK - s
                later = dec[b, t] * (cx[t][None] * row(gg, first, t) + later)
            return later

        later = lax.fori_loop(0, tokens // BACK, back, zero)
        for k in range(TILES):
            out1[c, message(k, 2 * o + 1), :] = later[k]

    def propagate(c):
        start, count = OCTETS[c]
        run = n // SUB
        settle(in1.at[c, pl.ds(0, 3 * count * (n - 1))], recv1.at[c])
        in1[c, slot(me, 3 * count), :] = out1[c, slot(me, 3 * count), :]
        line = lax.broadcasted_iota(jnp.int32, (SUB, LANES), 0)
        none = jnp.zeros((SUB, LANES), F32)

        def lines(j, r):
            return pl.ds(j * SUB + r, SUB, stride=run * SUB)

        def carried(total, last, shift, edge):
            carry = none
            for _ in range(SUB - 1):
                moved = pltpu.roll(total * carry + last, shift, axis=0)
                carry = jnp.where(line == edge, 0.0, moved)
            return carry

        for o in range(count):
            own = rt[
                (start + o) * octet + me // n_state,
                pl.ds(lax.rem(me, n_state), SUB, stride=0), :
            ]
            decays = [
                jnp.exp2(own * in1[c, lines(j, 2 * count + o), :]) for j in range(run)
            ]
            for r, order, shift, edge in (
                (2 * o, range(run), 1, 0), (2 * o + 1, reversed(range(run)), SUB - 1, SUB - 1)
            ):
                state, product = none, jnp.ones((SUB, LANES), F32)
                kept = []
                for j in order:
                    kept.append((j, state, product))
                    state = decays[j] * state + in1[c, lines(j, r), :]
                    product = decays[j] * product
                carry = carried(product, state, shift, edge)
                for j, local, reach in kept:
                    out2[c, lines(j, r), :] = local + reach * carry

    def returned(c):
        rows = 2 * OCTETS[c][1]
        settle(in2.at[c, pl.ds(0, rows * (n - 1))], recv2.at[c])
        in2[c, slot(me, rows), :] = out2[c, slot(me, rows), :]

    lane_group = lax.broadcasted_iota(jnp.int32, (SUB, LANES), 1) // width
    low_lanes = lax.broadcasted_iota(jnp.int32, (SUB // 2, LANES), 1) < LANES // 2

    def incoming(b, r):
        c, o, base = place(b)
        return jnp.stack([
            in2[c, pl.ds((base + k * n_state) * SUB + 2 * o + r, n_state, stride=SUB), :]
            for k in range(TILES)
        ])

    def gain(acc, t, part, fresh):
        acc[t] = part if fresh else acc[t] + part

    def restore(b):
        first = b * TILES
        fresh = isinstance(b, int) and b == 0

        def ahead(i, hidden):
            for s in range(AHEAD):
                t = i * AHEAD + s
                hs[t] = hidden
                hidden = dec[b, t] * hidden + bx[t][None] * row(uu, first, t)
                gain(accc, t, jnp.sum(row(gg, first, t) * hidden, axis=0), fresh)
            return hidden

        lax.fori_loop(0, tokens // AHEAD, ahead, incoming(b, 0))

    def fold_token(first, s, t, state, weighted, rates, fresh=False):
        one, two = state * bx[t][None], weighted * rates
        fold = pl.ds((s // SUB) * SUB * SUB + s % SUB, SUB, stride=SUB)
        for k in range(TILES):
            csp[k, fold, :] = one[k, :SUB] + one[k, SUB:]
            awp[k, fold, :] = two[k, :SUB] + two[k, SUB:]
        gain(accb, t, jnp.sum(state * row(uu, first, t), axis=0), fresh)

    def folded(ref, k):
        halves = []
        for h in range(PAIR // SUB):
            pieces = [
                ref[k, (h * SUB + s) * SUB : (h * SUB + s + 1) * SUB, :] for s in range(SUB)
            ]
            while len(pieces) > 1:
                pieces = [p + q for p, q in zip(pieces[::2], pieces[1::2])]
            halves.append(pieces[0])
        return jnp.concatenate(halves, axis=0)

    def finish(first, start):
        tok = pl.ds(pl.multiple_of(start, PAIR), PAIR)
        for k in range(TILES):
            coeff, weigh = folded(csp, k), folded(awp, k)
            lanes = lanes_at(first + k)
            x = xv[tok, lanes].astype(F32)
            giv[tok, lanes] = (dl[first + k, tok, :] * coeff).astype(giv.dtype)
            gsv[tok, lanes] = (x * coeff + LN2 * weigh).astype(gsv.dtype)

    def differentiate(b):
        first = b * TILES
        restore(b)

        def behind(i, carry):
            later, rate = carry
            rates = rt[pl.ds(first, TILES)]
            start = tokens - PAIR - i * PAIR
            for s in reversed(range(PAIR)):
                t = start + s
                state = cx[t][None] * row(gg, first, t) + later
                later = dec[b, t] * state
                weighted = later * hs[t]
                rate = rate + weighted * row(dl, first, t)
                fold_token(first, s, t, state, weighted, rates, first == 0)
            finish(first, start)
            return later, rate

        _, rate = lax.fori_loop(0, tokens // PAIR, behind, (incoming(b, 1), zero))
        for k in range(TILES):
            rs[first + k] = -rate[k]

    def sweep(b):
        first = b * TILES
        restore(b)

        def behind(i, carry):
            later, rate = carry
            for s in range(SWEEP):
                t = tokens - 1 - i * SWEEP - s
                state = cx[t][None] * row(gg, first, t) + later
                later = dec[b, t] * state
                weighted = later * hs[t]
                rate = rate + weighted * row(dl, first, t)
                dec[b, t] = state
                dec[b - DEFER, t] = weighted
            return later, rate

        _, rate = lax.fori_loop(0, tokens // SWEEP, behind, (incoming(b, 1), zero))
        for k in range(TILES):
            rs[first + k] = -rate[k]

    def gather(b):
        first = b * TILES

        def body(i):
            rates = rt[pl.ds(first, TILES)]
            start = i * PAIR
            for s in range(PAIR):
                t = start + s
                fold_token(first, s, t, dec[b, t], dec[b - DEFER, t], rates)
            finish(first, start)

        loop(0, tokens // PAIR, body)

    def give_rates(start, stop):
        for tile in range(start * TILES, stop * TILES):
            halves = (rs[tile, :SUB, :], rs[tile, SUB:, :])
            turned = [
                [v if s == 0 else pltpu.roll(v, s * width, axis=1) for s in range(parts)]
                for v in halves
            ]
            for j in range(parts):
                packed = turned[0][(0 - j) % parts]
                for g in range(1, parts):
                    packed = jnp.where(lane_group == g, turned[g % 2][(g - j) % parts], packed)
                pk[(tile - start * TILES) * parts + j] = packed
        for at in range((stop - start) * TILES * parts):
            out3[start * TILES * parts + at] = jnp.where(
                low_lanes, pk[at, : SUB // 2], pk[at, SUB // 2 :]
            )

        for at in range((stop - start) * TILES * parts):
            give3(start * TILES * parts + at)

    for b in range(3):
        summarize(b)
    pl.semaphore_wait(barrier, n - 1)
    everyone(partial(give1, 0))
    summarize(3)
    everyone(partial(give1, 1))
    for b in range(4, 6):
        summarize(b)
    propagate(0)
    everyone(partial(give2, 0))
    for b in range(6, 8):
        summarize(b)
    everyone(partial(give1, 2))
    propagate(1)
    everyone(partial(give2, 1))
    returned(0)
    differentiate(0)
    differentiate(1)
    propagate(2)
    everyone(partial(give2, 2))
    returned(1)
    differentiate(2)
    differentiate(3)
    give_rates(0, DEFER)
    returned(2)
    loop(DEFER, blocks, sweep)
    give_rates(DEFER, blocks)
    loop(DEFER, blocks, gather)
    in3[me] = out3[me]
    lane_sums(accb, gb_ref, tokens, n_state)
    lane_sums(accc, gc_ref, tokens, n_state)
    settle(in3.at[pl.ds(0, n)], recv3.at[0])
    blank = jnp.zeros((SUB // 2, LANES), F32)
    total = lax.fori_loop(0, n, lambda d, total: total + in3[d], blank, unroll=8)
    gr_ref[0:4, :] = total[:, :width]
    gr_ref[4:8, :] = total[:, 2 * width : 3 * width]
    gr_ref[8:12, :] = total[:, width : 2 * width]
    gr_ref[12:16, :] = total[:, 3 * width :]
    for c, (_, count) in enumerate(OCTETS):
        settle(out1.at[c, pl.ds(0, 3 * count * (n - 1))], send1.at[c])
        settle(out2.at[c, pl.ds(0, 2 * count * (n - 1))], send2.at[c])
    settle(out3.at[pl.ds(0, n)], send3.at[0])


def shards(n, inputs, step_sizes, cotangent, input_coeffs, output_coeffs, decay_rates):
    n_state, channels = decay_rates.shape
    tokens = inputs.shape[0]
    all_tiles = channels // LANES
    blocks = all_tiles // TILES
    parts = n // all_tiles
    wide = pltpu.VMEM((tokens, n_state, LANES), F32)
    flat = pltpu.VMEM((all_tiles, tokens, LANES), F32)
    fold = pltpu.VMEM((TILES, PAIR * SUB, LANES), F32)
    rows = pltpu.VMEM((tokens, channels), jnp.bfloat16)
    coefs = pltpu.VMEM((n_state, tokens), F32)
    vmem = pl.BlockSpec(memory_space=pltpu.VMEM)
    hbm = pl.BlockSpec(memory_space=pl.ANY)
    slots = pltpu.VMEM((len(OCTETS), n * SUB, LANES), F32)
    small = pltpu.VMEM((n + 1, SUB // 2, LANES), F32)
    each = pltpu.SemaphoreType.DMA((len(OCTETS),))
    one = pltpu.SemaphoreType.DMA((1,))
    outs = [
        jax.ShapeDtypeStruct((tokens, channels), jnp.bfloat16),
        jax.ShapeDtypeStruct((tokens, channels), jnp.bfloat16),
        jax.ShapeDtypeStruct((n_state, tokens), F32),
        jax.ShapeDtypeStruct((n_state, tokens), F32),
        jax.ShapeDtypeStruct((n_state, channels // n), F32),
    ]
    results = pl.pallas_call(
        partial(whole_kernel, n),
        name="whole",
        in_specs=[hbm] * 6,
        out_specs=[vmem] * 5,
        out_shape=[pltpu.VMEM(shape.shape, shape.dtype) for shape in outs],
        scratch_shapes=[
            rows, rows, rows, coefs, coefs, pltpu.VMEM((n_state, channels), F32),
            wide, wide, flat, flat, flat,
            pltpu.VMEM((blocks, tokens, TILES, n_state, LANES), F32),
            pltpu.VMEM((tokens, TILES, n_state, LANES), F32),
            wide, wide, fold, fold,
            pltpu.VMEM((all_tiles, n_state, LANES), F32),
            pltpu.VMEM((all_tiles, n_state, LANES), F32),
            pltpu.VMEM((DEFER * TILES * parts, SUB, LANES), F32),
            slots, slots, slots, slots, small, small,
            each, each, each, each, one, one,
            pltpu.SemaphoreType.DMA((3, blocks)),
            pltpu.SemaphoreType.DMA((3,)),
        ],
        compiler_params=pltpu.CompilerParams(
            collective_id=0, has_side_effects=True, vmem_limit_bytes=60 * 1024 * 1024
        ),
    )(inputs, step_sizes, cotangent, input_coeffs, output_coeffs, decay_rates)
    return pl.pallas_call(
        deliver,
        name="deliver",
        in_specs=[vmem] * 5,
        out_specs=[hbm] * 5,
        out_shape=outs,
        scratch_shapes=[pltpu.SemaphoreType.DMA((5, PIECES))],
        compiler_params=pltpu.CompilerParams(has_side_effects=False, vmem_limit_bytes=1024 * 1024),
    )(*[pltpu.with_memory_space_constraint(r, pltpu.VMEM) for r in results])


def solution(mesh):
    placed = (P("seq", None), P("seq", None), P("seq", None), P(None, "seq"), P(None, "seq"), P())
    return jax.shard_map(
        partial(shards, mesh.shape["seq"]),
        mesh=mesh,
        in_specs=placed,
        out_specs=(P("seq", None), P("seq", None), P(None, "seq"), P(None, "seq"), P(None, "seq")),
        check_vma=False,
    )
```
